32 devices in a mesh: node: 4 (over y, core), rep: 8 (over z, x).
Axes of the slice: x: 2, y: 2, z: 4, core: 2. Of those that a mesh axis runs over, the one named last changes fastest.
Arguments:
- tokens: bfloat16 [8192, 2048], P(('node', 'rep')), may hold values from -60 to 60
- cotangent: bfloat16 [8192, 512], P(('node', 'rep')), may hold values from -6 to 6
- value_weight: bfloat16 [2048, 512], P('node'), may hold values from -0.25 to 0.25
Outputs:
- input_grad: bfloat16 [8192, 2048], P(('node', 'rep'))
- update: float32 [2048, 512], P('node')
The draws below stay inside these ranges and needn't reach their ends.
All inputs are finite; a program needn't handle non-finite values.
Results may differ from the reference program's by a relative error of at most 0.025.
Values may be sent and summed in bfloat16 or wider, within the bound.
A program may use at most 64 MiB of HBM per device.

```python
import math
import jax
import jax.numpy as jnp
from jax import lax

DIN = 2048
KVH = 4
HD = 128
NS_ITERS = 5
TOK_DEV = 256
CV = 512
TOKENS = 8192
N_NODE = 4


def draw_tokens(key, part):
    key_values = jax.random.fold_in(key, 11)
    key_rough = jax.random.fold_in(key, 12)
    key_pair = jax.random.fold_in(key, 13)
    columns = jnp.arange(DIN, dtype=jnp.float32) / (DIN - 1)
    rough = jnp.exp(jax.random.uniform(key_rough, (DIN,), jnp.float32, jnp.log(0.7), jnp.log(1.4)))
    values = jnp.clip(jax.random.normal(key_values, (TOKENS, DIN), jnp.float32), -6.0, 6.0)
    rise = 3.0 ** columns
    offset = jax.random.randint(key_pair, (), 0, N_NODE)
    row_block = jnp.arange(TOKENS, dtype=jnp.int32) // TOK_DEV
    col_block = jnp.arange(DIN, dtype=jnp.int32) // (DIN // N_NODE)
    paired = ((row_block + offset) % N_NODE)[:, None] == col_block[None, :]
    spike = jnp.where(paired, 3.0, 1.0).astype(jnp.float32)
    return (values * spike * (rise * rough)[None, :]).astype(jnp.bfloat16)


def shard_levels(own_key, dims, pieces, smallest, high):
    loudness, own = 1.0, jax.random.fold_in(own_key, 6)
    for position, shards_of in pieces:
        draws = jnp.exp(jax.random.uniform(jax.random.fold_in(own, position), (shards_of,), jnp.float32, smallest / len(pieces), high / len(pieces)))
        loudness = loudness * jnp.repeat(draws, dims[position] // shards_of).reshape([-1 if axis == position else 1 for axis in range(len(dims))])
    return loudness


def noise(key, extent, deviation, most, split=(), kind=jnp.bfloat16):
    drawn = jax.random.normal(key, extent, jnp.float32) * deviation
    if len(split) > 0:
        drawn = shard_levels(key, extent, split, -0.22, 0.18) * drawn
    return jnp.clip(drawn, min=-most, max=most).astype(kind)


def setup_inputs(seed: int = 0) -> dict:
    seeds = jax.random.split(jax.random.key(seed), 4)
    tokens = draw_tokens(jax.random.fold_in(seeds[3], 71), 0)
    cotangent = noise(seeds[1], (TOKENS, CV), 1.0, 6.0, ((0, 32),))
    value_weight = noise(seeds[2], (DIN, CV), CV ** -0.5, 0.25, ((0, 4),))
    return {"tokens": tokens, "cotangent": cotangent, "value_weight": value_weight}


coef_a = 3.4445
coef_b = -4.775
coef_c = 2.0315
epsilon = 1e-07

def block_term(total, pair):
    rows_x, rows_c = pair
    term = jnp.einsum('td,tc->dc', rows_x.astype(jnp.float32), rows_c.astype(jnp.float32), precision=lax.Precision.HIGHEST)
    rounded = lax.optimization_barrier(term.astype(jnp.bfloat16))
    return (total + rounded.astype(jnp.float32), None)

def reference(tokens, cotangent, value_weight):
    width = cotangent.shape[1]
    input_grad = jnp.dot(cotangent, value_weight.T, preferred_element_type=jnp.float32).astype(jnp.bfloat16)
    blocks_x = tokens.reshape(-1, TOK_DEV, DIN)
    blocks_c = cotangent.reshape(-1, TOK_DEV, width)
    gradient, unused = lax.scan(block_term, jnp.zeros((DIN, width), jnp.float32), (blocks_x, blocks_c))
    blocks = gradient.reshape(DIN, KVH, HD)
    norms = jnp.sqrt(lax.optimization_barrier(jnp.sum(blocks * blocks, axis=(0, 2))))
    iterate = blocks / (norms[None, :, None] + epsilon)
    for step in range(NS_ITERS):
        gram = jnp.einsum('rhi,rhj->hij', iterate, iterate, precision=lax.Precision.HIGHEST)
        poly = coef_b * gram + coef_c * jnp.einsum('hij,hjk->hik', gram, gram, precision=lax.Precision.HIGHEST)
        iterate = coef_a * iterate + jnp.einsum('rhi,hij->rhj', iterate, poly, precision=lax.Precision.HIGHEST)
    update = 0.2 * math.sqrt(DIN) * iterate.reshape(DIN, width)
    return (input_grad, update)
```

```python
import functools
import math

import jax
import jax.numpy as jnp
from jax import lax
from jax.experimental import pallas as pl
from jax.experimental.pallas import tpu as pltpu
from jax.sharding import PartitionSpec as P

HD = 128
NS_ITERS = 5
NSUB = 1
TILE_ROWS = 16

coef_a = 3.4445
coef_b = -4.775
coef_c = 2.0315
epsilon = 1e-07

MESH = pl.DeviceIdType.MESH
F32, BF16 = jnp.float32, jnp.bfloat16


def mm_t(a, b):
    return lax.dot_general(a, b, (((0,), (0,)), ((), ())), preferred_element_type=F32)


def parts_of(a):
    hi = a.astype(BF16)
    lo = (a - hi.astype(F32)).astype(BF16)
    return hi, lo


def left_form(a):
    return jnp.concatenate(parts_of(a), axis=1)


def right_form(b):
    row = jnp.concatenate(parts_of(b), axis=1)
    return jnp.concatenate([row, row], axis=0)


def product(left, right):
    n = right.shape[1] // 2
    wide = jnp.dot(left, right, preferred_element_type=F32)
    return wide[:, :n] + wide[:, n:]


def kernel(cfg, tok_hbm, cot_hbm, w_hbm, ig_hbm, up_hbm, tok2, cot2, wall, acc1, send1, recv1, send2, recv2,
           zsend, zrecv, grad, gram_own, gram_in, igbuf, upbuf, lsem, ssem, rsem):
    depth, width, heads, zs = cfg
    din = tok_hbm.shape[1]
    tokens = tok_hbm.shape[0]
    block = din // 4
    half, quarter = block // 2, block // 4
    piece = quarter // zs
    cw = width // NSUB

    node, rep = lax.axis_index("node"), lax.axis_index("rep")
    y, c = node // 2, node % 2
    z, x = rep // 2, rep % 2
    partner = (y * 2 + 1 - c, rep)
    y_peer = ((1 - y) * 2 + c, rep)
    x_peer = (node, z * 2 + 1 - x)
    z_of = [(z + d) % zs for d in range(zs)]
    z_peer = [(node, z_of[d] * 2 + x) for d in range(zs)]

    local_copies = {}
    counts = {"l": 0, "r": 0}

    def local(src, dst):
        cp = pltpu.make_async_copy(src, dst, lsem.at[counts["l"]])
        counts["l"] += 1
        cp.start()
        return cp

    sends = []

    def remote(src, dst, peer):
        k = counts["r"]
        counts["r"] += 1
        cp = pltpu.make_async_remote_copy(src_ref=src, dst_ref=dst, send_sem=ssem.at[k], recv_sem=rsem.at[k],
                                          device_id=peer, device_id_type=MESH)
        cp.start()
        sends.append(cp)
        return cp

    def col(p, core):
        return pl.ds(pl.multiple_of((2 * p + core) * block, block), block)

    own_rows, other_rows = pl.ds(0, tokens), pl.ds(tokens, tokens)
    loads = [local(tok_hbm.at[:, col(p, c)], tok2.at[p, own_rows]) for p in range(2)]
    loads.append(local(cot_hbm, cot2.at[own_rows]))
    own_w = pl.ds(pl.multiple_of(node * block, block), block)
    load_w = local(w_hbm, wall.at[own_w])

    barrier = pltpu.get_barrier_semaphore()
    peers = [partner, y_peer, x_peer] + z_peer[1:]
    for peer in peers:
        pl.semaphore_signal(barrier, inc=1, device_id=peer, device_id_type=MESH)
    pl.semaphore_wait(barrier, len(peers))

    first = [remote(cot_hbm, cot2.at[other_rows], partner)]
    first += [remote(tok_hbm.at[:, col(p, 1 - c)], tok2.at[p, other_rows], partner) for p in range(2)]
    w_partner = remote(w_hbm, wall.at[own_w], partner)

    def dim(p, level):
        return (y, y_peer) if (p + level) % 2 == 0 else (x, x_peer)

    chunks = [(p, s) for s in range(NSUB) for p in range(2)]

    def cs(s):
        return pl.ds(s * cw, cw)

    for cp in loads:
        cp.wait()
    for cp in first:
        cp.wait_recv()

    st1, st2, stz, sg, sg2, sg1 = {}, {}, {}, {}, {}, {}
    for p, s in chunks:
        bit, peer = dim(p, 0)
        cols = pl.ds(pl.multiple_of((1 - bit) * half, half), half)
        send1[p, :, cs(s)] = mm_t(tok2[p, :, cols], cot2[:, cs(s)]).astype(BF16)
        st1[p, s] = remote(send1.at[p, :, cs(s)], recv1.at[p, :, cs(s)], peer)
    for p, s in chunks:
        bit, peer = dim(p, 0)
        cols = pl.ds(pl.multiple_of(bit * half, half), half)
        acc1[p, :, cs(s)] = mm_t(tok2[p, :, cols], cot2[:, cs(s)])

    def input_rows(n):
        rows = pl.ds(pl.multiple_of(n * block, block), block)
        out = lax.dot_general(cot2[0:tokens], wall[rows, :], (((1,), (1,)), ((), ())), preferred_element_type=F32)
        igbuf[:, rows] = out.astype(BF16)

    load_w.wait()
    input_rows(node)
    w_partner.wait_recv()
    input_rows(y * 2 + 1 - c)

    def base(p):
        return (2 * p + c) * block

    for p, s in chunks:
        st1[p, s].wait_recv()
        bit, peer = dim(p, 1)
        away = pl.ds(pl.multiple_of((1 - bit) * quarter, quarter), quarter)
        keep = pl.ds(pl.multiple_of(bit * quarter, quarter), quarter)
        send2[p, :, cs(s)] = (acc1[p, away, cs(s)] + recv1[p, away, cs(s)].astype(F32)).astype(BF16)
        st2[p, s] = remote(send2.at[p, :, cs(s)], recv2.at[p, :, cs(s)], peer)
        acc1[p, keep, cs(s)] = acc1[p, keep, cs(s)] + recv1[p, keep, cs(s)].astype(F32)
    w_y = remote(w_hbm, wall.at[own_w], y_peer)

    for p, s in chunks:
        st2[p, s].wait_recv()
        bit, peer = dim(p, 1)
        keep = pl.ds(pl.multiple_of(bit * quarter, quarter), quarter)
        total = acc1[p, keep, cs(s)] + recv2[p, :, cs(s)].astype(F32)
        acc1[p, keep, cs(s)] = total
        zsend[p, :, cs(s)] = total.astype(BF16)
        cps = []
        for d in range(1, zs):
            rows = pl.ds(pl.multiple_of(z_of[d] * piece, piece), piece)
            cps.append(remote(zsend.at[p, rows, cs(s)], zrecv.at[p, d - 1, :, cs(s)], z_peer[d]))
        stz[p, s] = cps

    for p, s in chunks:
        b0, _ = dim(p, 0)
        b1, _ = dim(p, 1)
        mine = pl.ds(pl.multiple_of(b1 * quarter + z * piece, piece), piece)
        total = acc1[p, mine, cs(s)]
        for d in range(1, zs):
            stz[p, s][d - 1].wait_recv()
            total = total + zrecv[p, d - 1, :, cs(s)].astype(F32)
        rows = pl.ds(pl.multiple_of(b0 * half + b1 * quarter + z * piece, piece), piece)
        grad[p, rows, cs(s)] = total.astype(BF16)
        sg[p, s] = [remote(grad.at[p, rows, cs(s)], grad.at[p, rows, cs(s)], z_peer[d]) for d in range(1, zs)]

    for p, s in chunks:
        for cp in sg[p, s]:
            cp.wait_recv()
        b0, _ = dim(p, 0)
        b1, peer = dim(p, 1)
        rows = pl.ds(pl.multiple_of(b0 * half + b1 * quarter, quarter), quarter)
        sg2[p, s] = remote(grad.at[p, rows, cs(s)], grad.at[p, rows, cs(s)], peer)
    w_y.wait_recv()
    y_w = pl.ds(pl.multiple_of(((1 - y) * 2 + c) * block, block), block)
    w_fwd = remote(wall.at[y_w], wall.at[y_w], partner)
    for p, s in chunks:
        sg2[p, s].wait_recv()
        b0, peer = dim(p, 0)
        rows = pl.ds(pl.multiple_of(b0 * half, half), half)
        sg1[p, s] = remote(grad.at[p, rows, cs(s)], grad.at[p, rows, cs(s)], peer)

    input_rows((1 - y) * 2 + c)
    w_fwd.wait_recv()
    input_rows((1 - y) * 2 + 1 - c)
    store_ig = local(igbuf, ig_hbm)

    def gram_of(h, p, bit):
        rows = pl.ds(pl.multiple_of(bit * half, half), half)
        g = grad[p, rows, h * HD:(h + 1) * HD]
        return mm_t(g, g)

    for h in range(heads):
        gram_own[h] = gram_of(h, 0, y) + gram_of(h, 1, x)
    for p, s in chunks:
        sg1[p, s].wait_recv()
    for h in range(heads):
        lower = gram_of(h, 0, 0) + gram_of(h, 0, 1)
        gram_own[h] = lower + (gram_of(h, 1, 0) + gram_of(h, 1, 1))
    cp_gram = remote(gram_own, gram_in, partner)
    cp_gram.wait_recv()

    ii = lax.broadcasted_iota(jnp.int32, (HD, HD), 0)
    jj = lax.broadcasted_iota(jnp.int32, (HD, HD), 1)
    eye = (ii == jj).astype(F32)
    grams, totals, scales = [], [None] * heads, []
    for h in range(heads):
        raw = gram_own[h] + gram_in[h]
        squares = jnp.sum(jnp.sum(raw * eye, axis=1, keepdims=True), axis=0, keepdims=True)
        inverse = 1.0 / (jnp.sqrt(squares) + epsilon)
        scales.append(inverse)
        grams.append(raw * inverse * inverse)
    for step in range(NS_ITERS):
        rights = [right_form(g) for g in grams]
        squared = [product(left_form(g), r) for g, r in zip(grams, rights)]
        factors = [coef_a * eye + coef_b * g + coef_c * q for g, q in zip(grams, squared)]
        forms = [right_form(f) for f in factors]
        if step + 1 < NS_ITERS:
            halfway = [product(left_form(g), f) for g, f in zip(grams, forms)]
        if step == 0:
            totals = factors
        else:
            totals = [product(left_form(t), f) for t, f in zip(totals, forms)]
        if step + 1 < NS_ITERS:
            grams = [product(left_form(g), f) for g, f in zip(halfway, forms)]

    for h in range(heads):
        scaled = totals[h] * (scales[h] * (0.2 * math.sqrt(din)))
        form = jnp.concatenate(parts_of(scaled), axis=1)
        upbuf[:, h * HD:(h + 1) * HD] = product(grad[y, :, h * HD:(h + 1) * HD], form)
    store_up = local(upbuf, up_hbm)
    for cp in sends:
        cp.wait_send()
    store_ig.wait()
    store_up.wait()


def fused(tokens, cotangent, value_weight, zs):
    tok, din = tokens.shape
    width = cotangent.shape[1]
    heads = width // HD
    block = din // 4
    half, quarter = block // 2, block // 4
    piece = quarter // zs
    nrem = 4 + 2 * NSUB * (1 + 1 + 2 * (zs - 1) + 1 + 1) + 3
    vm = pltpu.VMEM
    return pl.pallas_call(
        functools.partial(kernel, (tok, width, heads, zs)),
        out_shape=(jax.ShapeDtypeStruct((tok, din), BF16), jax.ShapeDtypeStruct((block, width), F32)),
        in_specs=[pl.BlockSpec(memory_space=pl.ANY)] * 3,
        out_specs=(pl.BlockSpec(memory_space=pl.ANY), pl.BlockSpec(memory_space=pl.ANY)),
        scratch_shapes=[
            vm((2, 2 * tok, block), BF16),
            vm((2 * tok, width), BF16),
            vm((din, width), BF16),
            vm((2, half, width), F32),
            vm((2, half, width), BF16),
            vm((2, half, width), BF16),
            vm((2, quarter, width), BF16),
            vm((2, quarter, width), BF16),
            vm((2, quarter, width), BF16),
            vm((2, zs - 1, piece, width), BF16),
            vm((2, block, width), BF16),
            vm((heads, HD, HD), F32),
            vm((heads, HD, HD), F32),
            vm((tok, din), BF16),
            vm((block, width), F32),
            pltpu.SemaphoreType.DMA((6,)),
            pltpu.SemaphoreType.DMA((nrem,)),
            pltpu.SemaphoreType.DMA((nrem,)),
        ],
        compiler_params=pltpu.CompilerParams(collective_id=0, has_side_effects=True, vmem_limit_bytes=56 * 1024 * 1024),
    )(tokens, cotangent, value_weight)


def general(tokens, cotangent, value_weight):
    width = value_weight.shape[1]
    din = tokens.shape[1]
    local_rows = value_weight.shape[0]
    heads = width // HD
    input_grad = lax.dot_general(
        cotangent,
        lax.all_gather(value_weight, "node", axis=0, tiled=True),
        (((1,), (1,)), ((), ())),
        preferred_element_type=F32,
    ).astype(BF16)
    partial_rows = lax.psum_scatter(
        lax.dot_general(tokens, cotangent, (((0,), (0,)), ((), ())), preferred_element_type=F32).astype(BF16),
        "node",
        scatter_dimension=0,
        tiled=True,
    ).astype(F32)
    gradient = lax.psum(partial_rows, "rep")
    blocks = gradient.reshape(local_rows, heads, HD)
    exact = functools.partial(jnp.einsum, precision=lax.Precision.HIGHEST)
    gram_raw = lax.psum(exact("rhi,rhj->hij", blocks, blocks), "node")
    divisor = jnp.sqrt(jnp.einsum("hii->h", gram_raw)) + epsilon
    gram = gram_raw / (divisor * divisor)[:, None, None]
    identity = jnp.broadcast_to(jnp.eye(HD, dtype=F32), (heads, HD, HD))
    total = identity
    for step in range(NS_ITERS):
        factor = coef_a * identity + coef_b * gram + coef_c * exact("hij,hjk->hik", gram, gram)
        total = exact("hij,hjk->hik", total, factor)
        if step + 1 < NS_ITERS:
            gram = exact("hji,hjk->hik", factor, exact("hij,hjk->hik", gram, factor))
    iterate = exact("rhi,hij->rhj", blocks / divisor[None, :, None], total)
    return input_grad, 0.2 * math.sqrt(din) * iterate.reshape(local_rows, width)


def solution(mesh):
    nodes, reps = mesh.shape["node"], mesh.shape["rep"]

    def per_device(tokens, cotangent, value_weight):
        zs = reps // 2
        pieces = nodes * 4 * zs
        fits = nodes == 4 and reps % 2 == 0 and zs > 1 and tokens.shape[1] % (pieces * TILE_ROWS) == 0
        if fits:
            return fused(tokens, cotangent, value_weight, zs)
        return general(tokens, cotangent, value_weight)

    return jax.shard_map(
        per_device,
        mesh=mesh,
        in_specs=(P(("node", "rep"), None), P(("node", "rep"), None), P("node", None)),
        out_specs=(P(("node", "rep"), None), P("node", None)),
        check_vma=False,
    )
```

```python
import functools
import math

import jax
import jax.numpy as jnp
from jax import lax
from jax.experimental import pallas as pl
from jax.experimental.pallas import tpu as pltpu
from jax.sharding import PartitionSpec as P

HD = 128
NS_ITERS = 5
NSUB = 2
TILE_ROWS = 16

coef_a = 3.4445
coef_b = -4.775
coef_c = 2.0315
epsilon = 1e-07

MESH = pl.DeviceIdType.MESH
F32, BF16 = jnp.float32, jnp.bfloat16


def mm_t(a, b):
    return lax.dot_general(a, b, (((0,), (0,)), ((), ())), preferred_element_type=F32)


def parts_of(a):
    hi = a.astype(BF16)
    lo = (a - hi.astype(F32)).astype(BF16)
    return hi, lo


def left_form(a):
    return jnp.concatenate(parts_of(a), axis=1)


def right_form(b):
    row = jnp.concatenate(parts_of(b), axis=1)
    return jnp.concatenate([row, row], axis=0)


def product(left, right):
    n = right.shape[1] // 2
    wide = jnp.dot(left, right, preferred_element_type=F32)
    return wide[:, :n] + wide[:, n:]


def kernel(cfg, tok_hbm, cot_hbm, w_hbm, igbuf, rows_ref, form_ref, tok_ref, cot_ref, w_ref, tokx, cotx, wall, acc1, away1, send1, recv1, send2,
           recv2, zsend, zrecv, grad, early, gram_own, gram_in, lsem, ssem, rsem):
    depth, width, heads, zs = cfg
    din = tok_ref.shape[1]
    tokens = tok_ref.shape[0]
    block = din // 4
    half, quarter = block // 2, block // 4
    piece = quarter // zs
    cw = width // NSUB

    node, rep = lax.axis_index("node"), lax.axis_index("rep")
    y, c = node // 2, node % 2
    z, x = rep // 2, rep % 2
    partner = (y * 2 + 1 - c, rep)
    y_peer = ((1 - y) * 2 + c, rep)
    x_peer = (node, z * 2 + 1 - x)
    z_of = [(z + d) % zs for d in range(zs)]
    z_peer = [(node, z_of[d] * 2 + x) for d in range(zs)]

    counts = [0]
    sends = []

    def remote(src, dst, peer):
        k = counts[0]
        counts[0] += 1
        cp = pltpu.make_async_remote_copy(src_ref=src, dst_ref=dst, send_sem=ssem.at[k], recv_sem=rsem.at[k],
                                          device_id=peer, device_id_type=MESH)
        cp.start()
        sends.append(cp)
        return cp

    def col(p, core, start=0, size=block):
        return pl.ds(pl.multiple_of((2 * p + core) * block + start, size), size)

    own_w = pl.ds(pl.multiple_of(node * block, block), block)

    pairs = ((cot_hbm, cot_ref), (tok_hbm, tok_ref), (w_hbm, w_ref))
    loads = [pltpu.make_async_copy(src, dst, lsem.at[i]) for i, (src, dst) in enumerate(pairs)]
    for cp in loads:
        cp.start()

    barrier = pltpu.get_barrier_semaphore()
    peers = [partner, y_peer, x_peer] + z_peer[1:]
    for peer in peers:
        pl.semaphore_signal(barrier, inc=1, device_id=peer, device_id_type=MESH)
    pl.semaphore_wait(barrier, len(peers))

    for cp in loads:
        cp.wait()
    first = [remote(cot_ref, cotx, partner)]
    first += [remote(tok_ref.at[:, col(p, 1 - c)], tokx.at[p], partner) for p in range(2)]

    def w_part(n, side, i):
        return pl.ds(pl.multiple_of(n * block + side * half + i * quarter, quarter), quarter)

    def send_w(i):
        rows = pl.ds(pl.multiple_of(x * half + i * quarter, quarter), quarter)
        return remote(w_ref.at[rows], wall.at[w_part(node, x, i)], y_peer)

    def relay_w(i):
        rows = w_part((1 - y) * 2 + c, x, i)
        return remote(wall.at[rows], wall.at[rows], x_peer)

    w_y = [send_w(0)]

    def dim(p, level):
        return (y, y_peer) if (p + level) % 2 == 0 else (x, x_peer)

    chunks = [(p, s) for s in range(NSUB) for p in range(2)]

    def cs(s):
        return pl.ds(s * cw, cw)

    def chip_sum(p, start):
        mine = mm_t(tok_ref[:, col(p, c, start, half)], cot_ref[...])
        return mine, pl.ds(pl.multiple_of(start, half), half)

    mine = {}
    for p in range(2):
        start = (1 - dim(p, 0)[0]) * half
        away1[p], mine[p] = chip_sum(p, start)
    st1, st2, stz, sg, sg2, sg1 = {}, {}, {}, {}, {}, {}
    first[0].wait_recv()
    for p in range(2):
        first[1 + p].wait_recv()
        send1[p] = (away1[p] + mm_t(tokx[p, :, mine[p]], cotx[...])).astype(BF16)
        for s in range(NSUB):
            st1[p, s] = remote(send1.at[p, :, cs(s)], recv1.at[p, :, cs(s)], dim(p, 0)[1])
    w_partner = remote(w_ref, wall.at[own_w], partner)
    for p in range(2):
        value, here = chip_sum(p, dim(p, 0)[0] * half)
        acc1[p] = value + mm_t(tokx[p, :, here], cotx[...])

    def input_rows(n, rows_of_w):
        rows = pl.ds(pl.multiple_of(n * block, block), block)
        out = lax.dot_general(cot_ref[...], rows_of_w, (((1,), (1,)), ((), ())), preferred_element_type=F32)
        igbuf[:, rows] = out.astype(BF16)

    def gathered(n):
        return wall[pl.ds(pl.multiple_of(n * block, block), block), :]

    input_rows(node, w_ref[...])
    w_partner.wait_recv()
    input_rows(y * 2 + 1 - c, gathered(y * 2 + 1 - c))

    for p, s in chunks:
        st1[p, s].wait_recv()
        bit, peer = dim(p, 1)
        away = pl.ds(pl.multiple_of((1 - bit) * quarter, quarter), quarter)
        keep = pl.ds(pl.multiple_of(bit * quarter, quarter), quarter)
        send2[p, :, cs(s)] = (acc1[p, away, cs(s)] + recv1[p, away, cs(s)].astype(F32)).astype(BF16)
        st2[p, s] = remote(send2.at[p, :, cs(s)], recv2.at[p, :, cs(s)], peer)
        acc1[p, keep, cs(s)] = acc1[p, keep, cs(s)] + recv1[p, keep, cs(s)].astype(F32)
    w_y.append(send_w(1))
    w_y[0].wait_recv()
    w_x = [relay_w(0)]

    for p, s in chunks:
        st2[p, s].wait_recv()
        bit, peer = dim(p, 1)
        keep = pl.ds(pl.multiple_of(bit * quarter, quarter), quarter)
        total = acc1[p, keep, cs(s)] + recv2[p, :, cs(s)].astype(F32)
        acc1[p, keep, cs(s)] = total
        zsend[p, :, cs(s)] = total.astype(BF16)
        cps = []
        for d in range(1, zs):
            rows = pl.ds(pl.multiple_of(z_of[d] * piece, piece), piece)
            cps.append(remote(zsend.at[p, rows, cs(s)], zrecv.at[p, d - 1, :, cs(s)], z_peer[d]))
        stz[p, s] = cps

    for p, s in chunks:
        b0, _ = dim(p, 0)
        b1, _ = dim(p, 1)
        mine = pl.ds(pl.multiple_of(b1 * quarter + z * piece, piece), piece)
        total = acc1[p, mine, cs(s)]
        for d in range(1, zs):
            stz[p, s][d - 1].wait_recv()
            total = total + zrecv[p, d - 1, :, cs(s)].astype(F32)
        rows = pl.ds(pl.multiple_of(b0 * half + b1 * quarter + z * piece, piece), piece)
        grad[p, rows, cs(s)] = total.astype(BF16)
        sg[p, s] = [remote(grad.at[p, rows, cs(s)], grad.at[p, rows, cs(s)], z_peer[d]) for d in range(1, zs)]

    w_y[1].wait_recv()
    w_x.append(relay_w(1))
    for p, s in chunks:
        for cp in sg[p, s]:
            cp.wait_recv()
        b0, _ = dim(p, 0)
        b1, peer = dim(p, 1)
        rows = pl.ds(pl.multiple_of(b0 * half + b1 * quarter, quarter), quarter)
        sg2[p, s] = remote(grad.at[p, rows, cs(s)], grad.at[p, rows, cs(s)], peer)
    for cp in w_x:
        cp.wait_recv()
    y_w = pl.ds(pl.multiple_of(((1 - y) * 2 + c) * block, block), block)
    w_fwd = remote(wall.at[y_w], wall.at[y_w], partner)
    for p, s in chunks:
        sg2[p, s].wait_recv()
        b0, peer = dim(p, 0)
        rows = pl.ds(pl.multiple_of(b0 * half, half), half)
        sg1[p, s] = remote(grad.at[p, rows, cs(s)], grad.at[p, rows, cs(s)], peer)

    input_rows((1 - y) * 2 + c, gathered((1 - y) * 2 + c))
    w_fwd.wait_recv()
    input_rows((1 - y) * 2 + 1 - c, gathered((1 - y) * 2 + 1 - c))

    def gram_of(h, p, bit):
        rows = pl.ds(pl.multiple_of(bit * half, half), half)
        g = grad[p, rows, h * HD:(h + 1) * HD]
        return mm_t(g, g)

    for h in range(heads):
        early[0, h] = gram_of(h, 0, y)
        early[1, h] = gram_of(h, 1, x)
    for p, s in chunks:
        sg1[p, s].wait_recv()
    for h in range(heads):
        gram_own[h] = (early[0, h] + gram_of(h, 0, 1 - y)) + (early[1, h] + gram_of(h, 1, 1 - x))
    cp_gram = remote(gram_own, gram_in, partner)
    rows_ref[...] = grad[y]
    cp_gram.wait_recv()

    ii = lax.broadcasted_iota(jnp.int32, (HD, HD), 0)
    jj = lax.broadcasted_iota(jnp.int32, (HD, HD), 1)
    eye = (ii == jj).astype(F32)
    grams, totals, scales = [], [None] * heads, []
    for h in range(heads):
        raw = gram_own[h] + gram_in[h]
        squares = jnp.sum(jnp.sum(raw * eye, axis=1, keepdims=True), axis=0, keepdims=True)
        inverse = 1.0 / (jnp.sqrt(squares) + epsilon)
        scales.append(inverse)
        grams.append(raw * inverse * inverse)
    for step in range(NS_ITERS):
        rights = [right_form(g) for g in grams]
        squared = [product(left_form(g), r) for g, r in zip(grams, rights)]
        factors = [coef_a * eye + coef_b * g + coef_c * q for g, q in zip(grams, squared)]
        forms = [right_form(f) for f in factors]
        if step + 1 < NS_ITERS:
            halfway = [product(left_form(g), f) for g, f in zip(grams, forms)]
        if step == 0:
            totals = factors
        else:
            totals = [product(left_form(t), f) for t, f in zip(totals, forms)]
        if step + 1 < NS_ITERS:
            grams = [product(left_form(g), f) for g, f in zip(halfway, forms)]

    for h in range(heads):
        scaled = totals[h] * (scales[h] * (0.2 * math.sqrt(din)))
        form_ref[h] = jnp.concatenate(parts_of(scaled), axis=1)
    for cp in sends:
        cp.wait_send()


def finish(ig_ref, rows_ref, form_ref, ig_out, up_out, upbuf, sems):
    heads = form_ref.shape[0]
    step = upbuf.shape[0] // 4
    copies = [pltpu.make_async_copy(ig_ref, ig_out, sems.at[0])]
    copies[0].start()
    for i in range(4):
        part = pl.ds(i * step, step)
        for h in range(heads):
            cols = pl.ds(h * HD, HD)
            upbuf[part, cols] = product(rows_ref[part, cols], form_ref[h])
        copies.append(pltpu.make_async_copy(upbuf.at[part], up_out.at[part], sems.at[i + 1]))
        copies[-1].start()
    for cp in copies:
        cp.wait()


def fused(tokens, cotangent, value_weight, zs):
    tok, din = tokens.shape
    width = cotangent.shape[1]
    heads = width // HD
    block = din // 4
    half, quarter = block // 2, block // 4
    piece = quarter // zs
    nrem = 4 + 2 * NSUB * (1 + 1 + 2 * (zs - 1) + 1 + 1) + 7
    vm = pltpu.VMEM
    held = pl.pallas_call(
        functools.partial(kernel, (tok, width, heads, zs)),
        out_shape=(
            jax.ShapeDtypeStruct((tok, din), BF16),
            jax.ShapeDtypeStruct((block, width), BF16),
            jax.ShapeDtypeStruct((heads, HD, 2 * HD), BF16),
        ),
        in_specs=[pl.BlockSpec(memory_space=pl.ANY)] * 3,
        out_specs=(pl.BlockSpec(memory_space=pltpu.VMEM),) * 3,
        scratch_shapes=[
            vm((tok, din), BF16),
            vm((tok, width), BF16),
            vm((block, width), BF16),
            vm((2, tok, block), BF16),
            vm((tok, width), BF16),
            vm((din, width), BF16),
            vm((2, half, width), F32),
            vm((2, half, width), F32),
            vm((2, half, width), BF16),
            vm((2, half, width), BF16),
            vm((2, quarter, width), BF16),
            vm((2, quarter, width), BF16),
            vm((2, quarter, width), BF16),
            vm((2, zs - 1, piece, width), BF16),
            vm((2, block, width), BF16),
            vm((2, heads, HD, HD), F32),
            vm((heads, HD, HD), F32),
            vm((heads, HD, HD), F32),
            pltpu.SemaphoreType.DMA((3,)),
            pltpu.SemaphoreType.DMA((nrem,)),
            pltpu.SemaphoreType.DMA((nrem,)),
        ],
        compiler_params=pltpu.CompilerParams(collective_id=0, has_side_effects=True, vmem_limit_bytes=24 * 1024 * 1024),
    )(*(pltpu.with_memory_space_constraint(a, pltpu.HBM) for a in (tokens, cotangent, value_weight)))
    return pl.pallas_call(
        finish,
        out_shape=(jax.ShapeDtypeStruct((tok, din), BF16), jax.ShapeDtypeStruct((block, width), F32)),
        in_specs=[pl.BlockSpec(memory_space=pltpu.VMEM)] * 3,
        out_specs=(pl.BlockSpec(memory_space=pltpu.HBM),) * 2,
        scratch_shapes=[vm((block, width), F32), pltpu.SemaphoreType.DMA((5,))],
        compiler_params=pltpu.CompilerParams(vmem_limit_bytes=8 * 1024 * 1024),
    )(*held)


def general(tokens, cotangent, value_weight):
    width = value_weight.shape[1]
    din = tokens.shape[1]
    local_rows = value_weight.shape[0]
    heads = width // HD
    input_grad = lax.dot_general(
        cotangent,
        lax.all_gather(value_weight, "node", axis=0, tiled=True),
        (((1,), (1,)), ((), ())),
        preferred_element_type=F32,
    ).astype(BF16)
    partial_rows = lax.psum_scatter(
        lax.dot_general(tokens, cotangent, (((0,), (0,)), ((), ())), preferred_element_type=F32).astype(BF16),
        "node",
        scatter_dimension=0,
        tiled=True,
    ).astype(F32)
    gradient = lax.psum(partial_rows, "rep")
    blocks = gradient.reshape(local_rows, heads, HD)
    exact = functools.partial(jnp.einsum, precision=lax.Precision.HIGHEST)
    gram_raw = lax.psum(exact("rhi,rhj->hij", blocks, blocks), "node")
    divisor = jnp.sqrt(jnp.einsum("hii->h", gram_raw)) + epsilon
    gram = gram_raw / (divisor * divisor)[:, None, None]
    identity = jnp.broadcast_to(jnp.eye(HD, dtype=F32), (heads, HD, HD))
    total = identity
    for step in range(NS_ITERS):
        factor = coef_a * identity + coef_b * gram + coef_c * exact("hij,hjk->hik", gram, gram)
        total = exact("hij,hjk->hik", total, factor)
        if step + 1 < NS_ITERS:
            gram = exact("hji,hjk->hik", factor, exact("hij,hjk->hik", gram, factor))
    iterate = exact("rhi,hij->rhj", blocks / divisor[None, :, None], total)
    return input_grad, 0.2 * math.sqrt(din) * iterate.reshape(local_rows, width)


def solution(mesh):
    nodes, reps = mesh.shape["node"], mesh.shape["rep"]

    def per_device(tokens, cotangent, value_weight):
        zs = reps // 2
        pieces = nodes * 4 * zs
        fits = nodes == 4 and reps % 2 == 0 and zs > 1 and tokens.shape[1] % (pieces * TILE_ROWS) == 0
        if fits:
            return fused(tokens, cotangent, value_weight, zs)
        return general(tokens, cotangent, value_weight)

    return jax.shard_map(
        per_device,
        mesh=mesh,
        in_specs=(P(("node", "rep"), None), P(("node", "rep"), None), P("node", None)),
        out_specs=(P(("node", "rep"), None), P("node", None)),
        check_vma=False,
    )
```

```python
import functools
import math

import jax
import jax.numpy as jnp
from jax import lax
from jax.experimental import pallas as pl
from jax.experimental.pallas import tpu as pltpu
from jax.sharding import PartitionSpec as P

HD = 128
NS_ITERS = 5
NSUB = 2
TILE_ROWS = 16

coef_a = 3.4445
coef_b = -4.775
coef_c = 2.0315
epsilon = 1e-07

MESH = pl.DeviceIdType.MESH
F32, BF16 = jnp.float32, jnp.bfloat16


def mm_t(a, b):
    return lax.dot_general(a, b, (((0,), (0,)), ((), ())), preferred_element_type=F32)


def parts_of(a):
    hi = a.astype(BF16)
    lo = (a - hi.astype(F32)).astype(BF16)
    return hi, lo


def left_form(a):
    return jnp.concatenate(parts_of(a), axis=1)


def right_form(b):
    row = jnp.concatenate(parts_of(b), axis=1)
    return jnp.concatenate([row, row], axis=0)


def product(left, right):
    n = right.shape[1] // 2
    wide = jnp.dot(left, right, preferred_element_type=F32)
    return wide[:, :n] + wide[:, n:]


def kernel(cfg, tok_hbm, cot_hbm, w_hbm, igbuf, rows_ref, form_ref, tok_ref, cot_ref, w_ref, tokx, cotx, wall, acc1, away1, send1, recv1, send2,
           recv2, zsend, zrecv, grad, early, gram_own, gram_in, lsem, ssem, rsem):
    depth, width, heads, zs = cfg
    din = tok_ref.shape[1]
    tokens = tok_ref.shape[0]
    block = din // 4
    half, quarter = block // 2, block // 4
    piece = quarter // zs
    cw = width // NSUB

    node, rep = lax.axis_index("node"), lax.axis_index("rep")
    y, c = node // 2, node % 2
    z, x = rep // 2, rep % 2
    partner = (y * 2 + 1 - c, rep)
    y_peer = ((1 - y) * 2 + c, rep)
    x_peer = (node, z * 2 + 1 - x)
    z_of = [(z + d) % zs for d in range(zs)]
    z_peer = [(node, z_of[d] * 2 + x) for d in range(zs)]

    counts = [0]
    sends = []

    def remote(src, dst, peer):
        k = counts[0]
        counts[0] += 1
        cp = pltpu.make_async_remote_copy(src_ref=src, dst_ref=dst, send_sem=ssem.at[k], recv_sem=rsem.at[k],
                                          device_id=peer, device_id_type=MESH)
        cp.start()
        sends.append(cp)
        return cp

    def col(p, core, start=0, size=block):
        return pl.ds(pl.multiple_of((2 * p + core) * block + start, size), size)

    own_w = pl.ds(pl.multiple_of(node * block, block), block)

    pairs = ((cot_hbm, cot_ref), (tok_hbm, tok_ref), (w_hbm, w_ref))
    loads = [pltpu.make_async_copy(src, dst, lsem.at[i]) for i, (src, dst) in enumerate(pairs)]
    for cp in loads:
        cp.start()

    barrier = pltpu.get_barrier_semaphore()
    peers = [partner, y_peer, x_peer] + z_peer[1:]
    for peer in peers:
        pl.semaphore_signal(barrier, inc=1, device_id=peer, device_id_type=MESH)
    pl.semaphore_wait(barrier, len(peers))

    for cp in loads[:2]:
        cp.wait()
    first = [remote(cot_ref, cotx, partner)]
    first += [remote(tok_ref.at[:, col(p, 1 - c)], tokx.at[p], partner) for p in range(2)]

    def w_part(n, side, i):
        return pl.ds(pl.multiple_of(n * block + side * half + i * quarter, quarter), quarter)

    def send_w(i):
        rows = pl.ds(pl.multiple_of(x * half + i * quarter, quarter), quarter)
        return remote(w_ref.at[rows], wall.at[w_part(node, x, i)], y_peer)

    def relay_w(i):
        rows = w_part((1 - y) * 2 + c, x, i)
        return remote(wall.at[rows], wall.at[rows], x_peer)

    loads[2].wait()
    w_y = [send_w(0)]

    def dim(p, level):
        return (y, y_peer) if (p + level) % 2 == 0 else (x, x_peer)

    chunks = [(p, s) for s in range(NSUB) for p in range(2)]

    def cs(s):
        return pl.ds(s * cw, cw)

    def chip_sum(p, start):
        mine = mm_t(tok_ref[:, col(p, c, start, half)], cot_ref[...])
        return mine, pl.ds(pl.multiple_of(start, half), half)

    mine = {}
    for p in range(2):
        start = (1 - dim(p, 0)[0]) * half
        away1[p], mine[p] = chip_sum(p, start)
    st1, st2, stz, sg, sg2, sg1 = {}, {}, {}, {}, {}, {}
    first[0].wait_recv()
    for p in range(2):
        first[1 + p].wait_recv()
        send1[p] = (away1[p] + mm_t(tokx[p, :, mine[p]], cotx[...])).astype(BF16)
        for s in range(NSUB):
            st1[p, s] = remote(send1.at[p, :, cs(s)], recv1.at[p, :, cs(s)], dim(p, 0)[1])
    w_partner = remote(w_ref, wall.at[own_w], partner)
    for p in range(2):
        value, here = chip_sum(p, dim(p, 0)[0] * half)
        acc1[p] = value + mm_t(tokx[p, :, here], cotx[...])

    def input_rows(n, rows_of_w):
        rows = pl.ds(pl.multiple_of(n * block, block), block)
        out = lax.dot_general(cot_ref[...], rows_of_w, (((1,), (1,)), ((), ())), preferred_element_type=F32)
        igbuf[:, rows] = out.astype(BF16)

    def gathered(n):
        return wall[pl.ds(pl.multiple_of(n * block, block), block), :]

    input_rows(node, w_ref[...])
    w_partner.wait_recv()
    input_rows(y * 2 + 1 - c, gathered(y * 2 + 1 - c))

    for p, s in chunks:
        st1[p, s].wait_recv()
        bit, peer = dim(p, 1)
        away = pl.ds(pl.multiple_of((1 - bit) * quarter, quarter), quarter)
        keep = pl.ds(pl.multiple_of(bit * quarter, quarter), quarter)
        send2[p, :, cs(s)] = (acc1[p, away, cs(s)] + recv1[p, away, cs(s)].astype(F32)).astype(BF16)
        st2[p, s] = remote(send2.at[p, :, cs(s)], recv2.at[p, :, cs(s)], peer)
        acc1[p, keep, cs(s)] = acc1[p, keep, cs(s)] + recv1[p, keep, cs(s)].astype(F32)
    w_y.append(send_w(1))
    w_y[0].wait_recv()
    w_x = [relay_w(0)]

    for p, s in chunks:
        st2[p, s].wait_recv()
        bit, peer = dim(p, 1)
        keep = pl.ds(pl.multiple_of(bit * quarter, quarter), quarter)
        total = acc1[p, keep, cs(s)] + recv2[p, :, cs(s)].astype(F32)
        acc1[p, keep, cs(s)] = total
        zsend[p, :, cs(s)] = total.astype(BF16)
        cps = []
        for d in range(1, zs):
            rows = pl.ds(pl.multiple_of(z_of[d] * piece, piece), piece)
            cps.append(remote(zsend.at[p, rows, cs(s)], zrecv.at[p, d - 1, :, cs(s)], z_peer[d]))
        stz[p, s] = cps

    for p, s in chunks:
        b0, _ = dim(p, 0)
        b1, _ = dim(p, 1)
        mine = pl.ds(pl.multiple_of(b1 * quarter + z * piece, piece), piece)
        total = acc1[p, mine, cs(s)]
        for d in range(1, zs):
            stz[p, s][d - 1].wait_recv()
            total = total + zrecv[p, d - 1, :, cs(s)].astype(F32)
        rows = pl.ds(pl.multiple_of(b0 * half + b1 * quarter + z * piece, piece), piece)
        grad[p, rows, cs(s)] = total.astype(BF16)
        sg[p, s] = [remote(grad.at[p, rows, cs(s)], grad.at[p, rows, cs(s)], z_peer[d]) for d in range(1, zs)]

    w_y[1].wait_recv()
    w_x.append(relay_w(1))
    for p, s in chunks:
        for cp in sg[p, s]:
            cp.wait_recv()
        b0, _ = dim(p, 0)
        b1, peer = dim(p, 1)
        rows = pl.ds(pl.multiple_of(b0 * half + b1 * quarter, quarter), quarter)
        sg2[p, s] = remote(grad.at[p, rows, cs(s)], grad.at[p, rows, cs(s)], peer)
    for cp in w_x:
        cp.wait_recv()
    y_w = pl.ds(pl.multiple_of(((1 - y) * 2 + c) * block, block), block)
    w_fwd = remote(wall.at[y_w], wall.at[y_w], partner)
    for p, s in chunks:
        sg2[p, s].wait_recv()
        b0, peer = dim(p, 0)
        rows = pl.ds(pl.multiple_of(b0 * half, half), half)
        sg1[p, s] = remote(grad.at[p, rows, cs(s)], grad.at[p, rows, cs(s)], peer)

    input_rows((1 - y) * 2 + c, gathered((1 - y) * 2 + c))
    w_fwd.wait_recv()
    input_rows((1 - y) * 2 + 1 - c, gathered((1 - y) * 2 + 1 - c))

    def gram_of(h, p, bit):
        rows = pl.ds(pl.multiple_of(bit * half, half), half)
        g = grad[p, rows, h * HD:(h + 1) * HD]
        return mm_t(g, g)

    for h in range(heads):
        early[0, h] = gram_of(h, 0, y)
        early[1, h] = gram_of(h, 1, x)
    per_sub = heads // NSUB
    cp_gram = []
    for s in range(NSUB):
        for p in range(2):
            sg1[p, s].wait_recv()
        for h in range(s * per_sub, (s + 1) * per_sub):
            gram_own[h] = (early[0, h] + gram_of(h, 0, 1 - y)) + (early[1, h] + gram_of(h, 1, 1 - x))
        these = pl.ds(s * per_sub, per_sub)
        cp_gram.append(remote(gram_own.at[these], gram_in.at[these], partner))
    rows_ref[...] = grad[y]
    for cp in cp_gram:
        cp.wait_recv()

    ii = lax.broadcasted_iota(jnp.int32, (HD, HD), 0)
    jj = lax.broadcasted_iota(jnp.int32, (HD, HD), 1)
    eye = (ii == jj).astype(F32)
    grams, totals, scales = [], [None] * heads, []
    for h in range(heads):
        raw = gram_own[h] + gram_in[h]
        squares = jnp.sum(jnp.sum(raw * eye, axis=1, keepdims=True), axis=0, keepdims=True)
        inverse = 1.0 / (jnp.sqrt(squares) + epsilon)
        scales.append(inverse)
        grams.append(raw * inverse * inverse)
    for step in range(NS_ITERS):
        rights = [right_form(g) for g in grams]
        squared = [product(left_form(g), r) for g, r in zip(grams, rights)]
        factors = [coef_a * eye + coef_b * g + coef_c * q for g, q in zip(grams, squared)]
        forms = [right_form(f) for f in factors]
        if step + 1 < NS_ITERS:
            halfway = [product(left_form(g), f) for g, f in zip(grams, forms)]
        if step == 0:
            totals = factors
        else:
            totals = [product(left_form(t), f) for t, f in zip(totals, forms)]
        if step + 1 < NS_ITERS:
            grams = [product(left_form(g), f) for g, f in zip(halfway, forms)]

    for h in range(heads):
        scaled = totals[h] * (scales[h] * (0.2 * math.sqrt(din)))
        form_ref[h] = jnp.concatenate(parts_of(scaled), axis=1)
    for cp in sends:
        cp.wait_send()


def finish(ig_ref, rows_ref, form_ref, ig_out, up_out, upbuf, sems):
    heads = form_ref.shape[0]
    step = upbuf.shape[0] // 4
    copies = [pltpu.make_async_copy(ig_ref, ig_out, sems.at[0])]
    copies[0].start()
    for i in range(4):
        part = pl.ds(i * step, step)
        for h in range(heads):
            cols = pl.ds(h * HD, HD)
            upbuf[part, cols] = product(rows_ref[part, cols], form_ref[h])
        copies.append(pltpu.make_async_copy(upbuf.at[part], up_out.at[part], sems.at[i + 1]))
        copies[-1].start()
    for cp in copies:
        cp.wait()


def fused(tokens, cotangent, value_weight, zs):
    tok, din = tokens.shape
    width = cotangent.shape[1]
    heads = width // HD
    block = din // 4
    half, quarter = block // 2, block // 4
    piece = quarter // zs
    nrem = 4 + 2 * NSUB * (1 + 1 + 2 * (zs - 1) + 1 + 1) + 6 + NSUB
    vm = pltpu.VMEM
    held = pl.pallas_call(
        functools.partial(kernel, (tok, width, heads, zs)),
        out_shape=(
            jax.ShapeDtypeStruct((tok, din), BF16),
            jax.ShapeDtypeStruct((block, width), BF16),
            jax.ShapeDtypeStruct((heads, HD, 2 * HD), BF16),
        ),
        in_specs=[pl.BlockSpec(memory_space=pl.ANY)] * 3,
        out_specs=(pl.BlockSpec(memory_space=pltpu.VMEM),) * 3,
        scratch_shapes=[
            vm((tok, din), BF16),
            vm((tok, width), BF16),
            vm((block, width), BF16),
            vm((2, tok, block), BF16),
            vm((tok, width), BF16),
            vm((din, width), BF16),
            vm((2, half, width), F32),
            vm((2, half, width), F32),
            vm((2, half, width), BF16),
            vm((2, half, width), BF16),
            vm((2, quarter, width), BF16),
            vm((2, quarter, width), BF16),
            vm((2, quarter, width), BF16),
            vm((2, zs - 1, piece, width), BF16),
            vm((2, block, width), BF16),
            vm((2, heads, HD, HD), F32),
            vm((heads, HD, HD), F32),
            vm((heads, HD, HD), F32),
            pltpu.SemaphoreType.DMA((3,)),
            pltpu.SemaphoreType.DMA((nrem,)),
            pltpu.SemaphoreType.DMA((nrem,)),
        ],
        compiler_params=pltpu.CompilerParams(collective_id=0, has_side_effects=True, vmem_limit_bytes=24 * 1024 * 1024),
    )(*(pltpu.with_memory_space_constraint(a, pltpu.HBM) for a in (tokens, cotangent, value_weight)))
    return pl.pallas_call(
        finish,
        out_shape=(jax.ShapeDtypeStruct((tok, din), BF16), jax.ShapeDtypeStruct((block, width), F32)),
        in_specs=[pl.BlockSpec(memory_space=pltpu.VMEM)] * 3,
        out_specs=(pl.BlockSpec(memory_space=pltpu.HBM),) * 2,
        scratch_shapes=[vm((block, width), F32), pltpu.SemaphoreType.DMA((5,))],
        compiler_params=pltpu.CompilerParams(vmem_limit_bytes=8 * 1024 * 1024),
    )(*held)


def general(tokens, cotangent, value_weight):
    width = value_weight.shape[1]
    din = tokens.shape[1]
    local_rows = value_weight.shape[0]
    heads = width // HD
    input_grad = lax.dot_general(
        cotangent,
        lax.all_gather(value_weight, "node", axis=0, tiled=True),
        (((1,), (1,)), ((), ())),
        preferred_element_type=F32,
    ).astype(BF16)
    partial_rows = lax.psum_scatter(
        lax.dot_general(tokens, cotangent, (((0,), (0,)), ((), ())), preferred_element_type=F32).astype(BF16),
        "node",
        scatter_dimension=0,
        tiled=True,
    ).astype(F32)
    gradient = lax.psum(partial_rows, "rep")
    blocks = gradient.reshape(local_rows, heads, HD)
    exact = functools.partial(jnp.einsum, precision=lax.Precision.HIGHEST)
    gram_raw = lax.psum(exact("rhi,rhj->hij", blocks, blocks), "node")
    divisor = jnp.sqrt(jnp.einsum("hii->h", gram_raw)) + epsilon
    gram = gram_raw / (divisor * divisor)[:, None, None]
    identity = jnp.broadcast_to(jnp.eye(HD, dtype=F32), (heads, HD, HD))
    total = identity
    for step in range(NS_ITERS):
        factor = coef_a * identity + coef_b * gram + coef_c * exact("hij,hjk->hik", gram, gram)
        total = exact("hij,hjk->hik", total, factor)
        if step + 1 < NS_ITERS:
            gram = exact("hji,hjk->hik", factor, exact("hij,hjk->hik", gram, factor))
    iterate = exact("rhi,hij->rhj", blocks / divisor[None, :, None], total)
    return input_grad, 0.2 * math.sqrt(din) * iterate.reshape(local_rows, width)


def solution(mesh):
    nodes, reps = mesh.shape["node"], mesh.shape["rep"]

    def per_device(tokens, cotangent, value_weight):
        zs = reps // 2
        pieces = nodes * 4 * zs
        fits = nodes == 4 and reps % 2 == 0 and zs > 1 and tokens.shape[1] % (pieces * TILE_ROWS) == 0
        if fits:
            return fused(tokens, cotangent, value_weight, zs)
        return general(tokens, cotangent, value_weight)

    return jax.shard_map(
        per_device,
        mesh=mesh,
        in_specs=(P(("node", "rep"), None), P(("node", "rep"), None), P("node", None)),
        out_specs=(P(("node", "rep"), None), P("node", None)),
        check_vma=False,
    )
```
